128 devices in a mesh: rows: 8 (over x, core), cols: 16 (over z, y).
Axes of the slice: x: 4, y: 4, z: 4, core: 2. Of those that a mesh axis runs over, the one named last changes fastest.
Arguments:
- w_gate: bfloat16 [3584, 14336], P('rows', 'cols'), may hold values from -0.09375 to 0.09375
- low_gate: bfloat16 [3584, 64], P('rows'), may hold values from -0.09375 to 0.09375
- high_gate: bfloat16 [64, 14336], P(None, 'cols'), may hold values from -0.75 to 0.75
- w_up: bfloat16 [3584, 14336], P('rows', 'cols'), may hold values from -0.09375 to 0.09375
- low_up: bfloat16 [3584, 64], P('rows'), may hold values from -0.09375 to 0.09375
- high_up: bfloat16 [64, 14336], P(None, 'cols'), may hold values from -0.75 to 0.75
- w_down: bfloat16 [14336, 3584], P('cols', 'rows'), may hold values from -0.046875 to 0.046875
- low_down: bfloat16 [14336, 64], P('cols'), may hold values from -0.046875 to 0.046875
- high_down: bfloat16 [64, 3584], P(None, 'rows'), may hold values from -0.75 to 0.75
- norm_train: float32 [3584], P(('rows', 'cols')), may hold values from 0.25 to 1.75
- norm_step: float32 [3584], P(('rows', 'cols')), may hold values from -0.3 to 0.3
Outputs:
- serving_gate: bfloat16 [3584, 14336], P(None, 'cols')
- serving_up: bfloat16 [3584, 14336], P(None, 'cols')
- serving_down: bfloat16 [14336, 3584], P('cols')
- serve_norm: bfloat16 [3584], replicated
The draws below stay inside these ranges and needn't reach their ends.
All inputs are finite; a program needn't handle non-finite values.
Results may differ from the reference program's by a relative error of at most 0.001.
Values may be sent and summed in bfloat16 or wider, within the bound.
No kernel may reach another device: no remote copies, remote signals or barrier semaphores. Data moves between devices by JAX's collectives and lax.ppermute only.
A program may use at most 128 MiB of HBM per device.

```python
import jax
import jax.numpy as jnp

D_MODEL = 3584
D_INNER = 14336
RANK = 64


def steps_of(key, dims, shards, least, top_value):
    gain, own = 1.0, jax.random.fold_in(key, 6)
    for position, blocks in shards:
        steps = jnp.exp(jax.random.uniform(jax.random.fold_in(own, position), (blocks,), jnp.float32, least / len(shards), top_value / len(shards)))
        gain = gain * jnp.repeat(steps, dims[position] // blocks).reshape([-1 if axis == position else 1 for axis in range(len(dims))])
    return gain


def normal_values(stream_key, dims, spread, reach, cuts=(), kind=jnp.bfloat16):
    entries = spread * jax.random.normal(stream_key, dims, jnp.float32)
    if cuts:
        entries = entries * steps_of(stream_key, dims, cuts, -0.22, 0.18)
    return jnp.clip(entries, -reach, reach).astype(kind)


def setup_inputs(seed: int = 0) -> dict:
    streams_of = jax.random.split(jax.random.key(seed), 12)
    return {
        "w_gate": normal_values(streams_of[0], (D_MODEL, D_INNER), D_MODEL ** -0.5, 0.09375, ((0, 8), (1, 16))),
        "low_gate": normal_values(streams_of[1], (D_MODEL, RANK), D_MODEL ** -0.5, 0.09375, ((0, 8),)),
        "high_gate": normal_values(streams_of[2], (RANK, D_INNER), RANK ** -0.5, 0.75, ((1, 16),)),
        "w_up": normal_values(streams_of[3], (D_MODEL, D_INNER), D_MODEL ** -0.5, 0.09375, ((0, 8), (1, 16))),
        "low_up": normal_values(streams_of[4], (D_MODEL, RANK), D_MODEL ** -0.5, 0.09375, ((0, 8),)),
        "high_up": normal_values(streams_of[5], (RANK, D_INNER), RANK ** -0.5, 0.75, ((1, 16),)),
        "w_down": normal_values(streams_of[6], (D_INNER, D_MODEL), D_INNER ** -0.5, 0.046875, ((0, 16), (1, 8))),
        "low_down": normal_values(streams_of[7], (D_INNER, RANK), D_INNER ** -0.5, 0.046875, ((0, 16),)),
        "high_down": normal_values(streams_of[8], (RANK, D_MODEL), RANK ** -0.5, 0.75, ((1, 8),)),
        "norm_train": jnp.clip(1.0 + 0.15 * jax.random.normal(streams_of[9], (D_MODEL,), jnp.float32), 0.25, 1.75),
        "norm_step": jnp.clip(jax.random.uniform(streams_of[10], (D_MODEL,), jnp.float32, -0.3, 0.3) * steps_of(streams_of[10], (D_MODEL,), ((0, 128),), -0.4, 0.0), -0.3, 0.3),
    }


mix_rate = 0.5


def reference(w_gate, low_gate, high_gate, w_up, low_up, high_up, w_down, low_down, high_down, norm_train, norm_step):
    whole_gate = w_gate.astype(jnp.float32) + mix_rate * jnp.dot(low_gate, high_gate, preferred_element_type=jnp.float32)
    whole_up = w_up.astype(jnp.float32) + mix_rate * jnp.dot(low_up, high_up, preferred_element_type=jnp.float32)
    whole_down = w_down.astype(jnp.float32) + mix_rate * jnp.dot(low_down, high_down, preferred_element_type=jnp.float32)
    serving_gate = whole_gate.astype(jnp.bfloat16)
    serving_up = whole_up.astype(jnp.bfloat16)
    serving_down = whole_down.astype(jnp.bfloat16)
    serve_norm = (norm_train + norm_step).astype(jnp.bfloat16)
    return serving_gate, serving_up, serving_down, serve_norm
```

```python
import jax
import jax.numpy as jnp
from jax import lax
from jax.experimental import pallas as pl
from jax.experimental.pallas import tpu as pltpu
from jax.sharding import Mesh
from jax.sharding import PartitionSpec as P

ROWS = ("rows_0", "rows_1")
ROWS_COLS = ("rows_0", "rows_1", "cols_0", "cols_1")
COLS = ("cols_0", "cols_1")

mix_rate = 0.5

RIGHT = [(i, (i + 1) % 4) for i in range(4)]
LEFT = [(i, (i + 3) % 4) for i in range(4)]
ACROSS = [(i, (i + 2) % 4) for i in range(4)]
SWAP = [(0, 1), (1, 0)]


def right(a):
    return lax.ppermute(a, "rows_0", RIGHT)


def left(a):
    return lax.ppermute(a, "rows_0", LEFT)


def swap(a):
    return lax.ppermute(a, "rows_1", SWAP)


def tied(a, *others):
    return lax.optimization_barrier((a, *others))[0]


def merged(w, low, high):
    whole = w.astype(jnp.float32) + mix_rate * jnp.dot(low, high, preferred_element_type=jnp.float32)
    return whole.astype(jnp.bfloat16)


def place(shape, pieces, spots, name, into=None):
    n = len(pieces)
    by_rows = shape[1] == 896

    def kernel(*refs):
        out = refs[-2]
        sems = refs[-1]
        x, c = lax.axis_index("rows_0"), lax.axis_index("rows_1")
        copies = []
        for k in range(n):
            step, other, first = spots[k]
            xs = lax.rem(x + step, 4)
            cs = 1 - c if other else c
            if by_rows:
                row, col = (xs * 2 + cs) * 448 + first, 0
            else:
                row, col = cs * 448 + first, pl.multiple_of(xs * 896, 128)
            row = pl.multiple_of(row, 32)
            target = out.at[pl.ds(row, pieces[k].shape[0]), pl.ds(col, 896)]
            copies.append(pltpu.make_async_copy(refs[k], target, sems.at[k]))
        for copy in copies:
            copy.start()
        for copy in copies:
            copy.wait()

    operands = list(pieces)
    in_specs = [pl.BlockSpec(memory_space=pltpu.VMEM)] * n
    aliases = {}
    if into is not None:
        operands.append(into)
        in_specs.append(pl.BlockSpec(memory_space=pl.ANY))
        aliases = {n: 0}
    total = sum(p.size * 2 for p in pieces)
    return pl.pallas_call(
        kernel,
        out_shape=jax.ShapeDtypeStruct(shape, jnp.bfloat16),
        in_specs=in_specs,
        out_specs=pl.BlockSpec(memory_space=pl.ANY),
        scratch_shapes=[pltpu.SemaphoreType.DMA((n,))],
        input_output_aliases=aliases,
        compiler_params=pltpu.CompilerParams(vmem_limit_bytes=total + (1 << 20)),
        cost_estimate=pl.CostEstimate(flops=total, bytes_accessed=2 * total, transcendentals=0),
        name=name,
    )(*operands)


def summed(a, axis):
    others = [lax.ppermute(a, axis, p) for p in (RIGHT, LEFT, ACROSS)]
    return a + others[0] + others[1] + others[2]


def local(
    w_gate,
    low_gate,
    high_gate,
    w_up,
    low_up,
    high_up,
    w_down,
    low_down,
    high_down,
    norm_train,
    norm_step,
):
    core = lax.axis_index("rows_1")
    gate = merged(w_gate, low_gate, high_gate)
    gate_l, gate_r = right(gate), left(gate)
    up = merged(tied(w_up, gate), low_up, high_up)
    up_l, up_r = right(up), left(up)
    down = merged(tied(w_down, up), low_down, high_down)
    halves = down.reshape(2, 448, 448)
    mine = lax.dynamic_index_in_dim(halves, core, 0, keepdims=False)
    theirs = lax.dynamic_index_in_dim(halves, 1 - core, 0, keepdims=False)
    got = swap(theirs)
    first = jnp.where(core == 0, mine, got)
    second = jnp.where(core == 0, got, mine)
    pair = jnp.concatenate([first, second], axis=1)
    pair_l, pair_r = right(pair), left(pair)

    spot = lax.axis_index(ROWS_COLS) * 28
    own = (norm_train + norm_step).astype(jnp.bfloat16)
    norm = lax.dynamic_update_slice(jnp.zeros((3584,), jnp.bfloat16), own, (spot,))
    norm = norm + swap(norm)
    norm = summed(norm, "cols_1")
    norm = summed(norm, "cols_0")
    serve_norm = summed(norm, "rows_0")

    gate_t = right(gate_l)
    up_t = left(up_r)
    pair_ta = right(pair_l[:224])
    pair_tb = left(pair_r[224:])

    def both(pieces):
        return [*pieces, *(swap(p) for p in pieces)]

    near = [(0, False, 0), (3, False, 0), (1, False, 0), (0, True, 0), (3, True, 0), (1, True, 0)]
    far = [(2, False, 0), (2, True, 0)]
    far_down = [(2, False, 0), (2, False, 224), (2, True, 0), (2, True, 224)]
    serving_gate = place((3584, 896), both([gate, gate_l, gate_r]), near, "gate_near")
    serving_up = place((3584, 896), both([up, up_l, up_r]), near, "up_near")
    serving_down = place((896, 3584), both([pair, pair_l, pair_r]), near, "down_near")
    serving_gate = place((3584, 896), both([gate_t]), far, "gate_far", serving_gate)
    serving_up = place((3584, 896), both([up_t]), far, "up_far", serving_up)
    serving_down = place((896, 3584), both([pair_ta, pair_tb]), far_down, "down_far", serving_down)
    return (serving_gate, serving_up, serving_down, serve_norm)


def solution(mesh):
    torus = Mesh(mesh.devices.reshape(4, 2, 4, 4), ("rows_0", "rows_1", "cols_0", "cols_1"))
    placed = (
        P(ROWS, COLS),
        P(ROWS, None),
        P(None, COLS),
        P(ROWS, COLS),
        P(ROWS, None),
        P(None, COLS),
        P(COLS, ROWS),
        P(COLS, None),
        P(None, ROWS),
        P(ROWS_COLS),
        P(ROWS_COLS),
    )
    return jax.shard_map(
        local,
        mesh=torus,
        in_specs=placed,
        out_specs=(P(None, COLS), P(None, COLS), P(COLS, None), P()),
        check_vma=False,
    )
```

```python
import jax
import jax.numpy as jnp
from jax import lax
from jax.experimental import pallas as pl
from jax.experimental.pallas import tpu as pltpu
from jax.sharding import Mesh
from jax.sharding import PartitionSpec as P

ROWS = ("rows_0", "rows_1")
ROWS_COLS = ("rows_0", "rows_1", "cols_0", "cols_1")
COLS = ("cols_0", "cols_1")

mix_rate = 0.5

RIGHT = [(i, (i + 1) % 4) for i in range(4)]
LEFT = [(i, (i + 3) % 4) for i in range(4)]
ACROSS = [(i, (i + 2) % 4) for i in range(4)]
SWAP = [(0, 1), (1, 0)]


def right(a):
    return lax.ppermute(a, "rows_0", RIGHT)


def left(a):
    return lax.ppermute(a, "rows_0", LEFT)


def swap(a):
    return lax.ppermute(a, "rows_1", SWAP)


def tied(a, *others):
    return lax.optimization_barrier((a, *others))[0]


def merged(w, low, high):
    whole = w.astype(jnp.float32) + mix_rate * jnp.dot(low, high, preferred_element_type=jnp.float32)
    return whole.astype(jnp.bfloat16)


def place(shape, pieces, spots, into=None):
    n = len(pieces)
    by_rows = shape[1] == 896

    def kernel(*refs):
        out = refs[-2]
        sems = refs[-1]
        x, c = lax.axis_index("rows_0"), lax.axis_index("rows_1")
        copies = []
        for k in range(n):
            step, other, first = spots[k]
            xs = lax.rem(x + step, 4)
            cs = 1 - c if other else c
            if by_rows:
                row, col = (xs * 2 + cs) * 448 + first, 0
            else:
                row, col = cs * 448 + first, pl.multiple_of(xs * 896, 128)
            row = pl.multiple_of(row, 32)
            target = out.at[pl.ds(row, pieces[k].shape[0]), pl.ds(col, 896)]
            copies.append(pltpu.make_async_copy(refs[k], target, sems.at[k]))
        for copy in copies:
            copy.start()
        for copy in copies:
            copy.wait()

    operands = list(pieces)
    in_specs = [pl.BlockSpec(memory_space=pltpu.VMEM)] * n
    aliases = {}
    if into is not None:
        operands.append(into)
        in_specs.append(pl.BlockSpec(memory_space=pl.ANY))
        aliases = {n: 0}
    total = sum(p.size * 2 for p in pieces)
    return pl.pallas_call(
        kernel,
        out_shape=jax.ShapeDtypeStruct(shape, jnp.bfloat16),
        in_specs=in_specs,
        out_specs=pl.BlockSpec(memory_space=pl.ANY),
        scratch_shapes=[pltpu.SemaphoreType.DMA((n,))],
        input_output_aliases=aliases,
        compiler_params=pltpu.CompilerParams(vmem_limit_bytes=total + (1 << 20)),
        cost_estimate=pl.CostEstimate(flops=total, bytes_accessed=2 * total, transcendentals=0),
    )(*operands)


def summed(a, axis):
    others = []
    for pairs in (RIGHT, LEFT, ACROSS):
        others.append(lax.ppermute(a, axis, pairs))
    return a + others[0] + others[1] + others[2]


def local(
    w_gate,
    low_gate,
    high_gate,
    w_up,
    low_up,
    high_up,
    w_down,
    low_down,
    high_down,
    norm_train,
    norm_step,
):
    core = lax.axis_index("rows_1")
    gate = merged(w_gate, low_gate, high_gate)
    gate_l, gate_r = right(gate), left(gate)
    up = merged(tied(w_up, gate), low_up, high_up)
    up_l, up_r = right(up), left(up)
    down = merged(tied(w_down, up), low_down, high_down)
    halves = down.reshape(2, 448, 448)
    mine = lax.dynamic_index_in_dim(halves, core, 0, keepdims=False)
    theirs = lax.dynamic_index_in_dim(halves, 1 - core, 0, keepdims=False)
    got = swap(theirs)
    first = jnp.where(core == 0, mine, got)
    second = jnp.where(core == 0, got, mine)
    pair = jnp.concatenate([first, second], axis=1)
    pair_l, pair_r = right(pair), left(pair)

    spot = lax.axis_index(ROWS_COLS) * 28
    own = (norm_train + norm_step).astype(jnp.bfloat16)
    norm = lax.dynamic_update_slice(jnp.zeros((3584,), jnp.bfloat16), tied(own, pair), (spot,))
    norm = norm + swap(norm)
    norm = summed(norm, "cols_1")

    gate_l = tied(gate_l, norm)
    up_r = tied(up_r, norm)
    gate_t = right(gate_l)
    up_t = left(up_r)
    gate_s, up_s, pair_s = swap(gate), swap(up), swap(pair)
    gate_ls, up_rs = swap(gate_l), swap(up_r)
    norm = summed(tied(norm, gate_l, up_r), "cols_0")

    gate_r = tied(gate_r, norm)
    up_l = tied(up_l, norm)
    gate_rs, up_ls = swap(gate_r), swap(up_l)
    serve_norm = summed(tied(norm, gate_r, up_l), "rows_0")

    near = [(0, False, 0), (3, False, 0), (1, False, 0), (0, True, 0), (3, True, 0), (1, True, 0)]
    far = [(2, False, 0), (2, True, 0)]
    serving_gate = place((3584, 896), [gate, gate_l, gate_r, gate_s, gate_ls, gate_rs], near)
    serving_up = place((3584, 896), [up, up_l, up_r, up_s, up_ls, up_rs], near)
    pair_l = tied(pair_l, serving_gate, serving_up)
    pair_r = tied(pair_r, serving_gate, serving_up)
    pair_ta = right(pair_l[:224])
    pair_tb = left(pair_r[224:])
    pair_ls, pair_rs = swap(pair_l), swap(pair_r)
    serving_down = place((896, 3584), [pair, pair_l, pair_r, pair_s, pair_ls, pair_rs], near)
    gate_t = tied(gate_t, serving_down)
    up_t = tied(up_t, serving_down)
    serving_gate = place((3584, 896), [gate_t, swap(gate_t)], far, serving_gate)
    serving_up = place((3584, 896), [up_t, swap(up_t)], far, serving_up)
    pair_ta = tied(pair_ta, serving_gate, serving_up, serve_norm)
    pair_tb = tied(pair_tb, serving_gate, serving_up, serve_norm)
    pair_tas, pair_tbs = swap(pair_ta), swap(pair_tb)
    serving_down = place((896, 3584), [pair_ta, pair_tb], [(2, False, 0), (2, False, 224)], serving_down)
    serving_down = place((896, 3584), [pair_tas, pair_tbs], [(2, True, 0), (2, True, 224)], serving_down)
    return (serving_gate, serving_up, serving_down, serve_norm)


def solution(mesh):
    torus = Mesh(mesh.devices.reshape(4, 2, 4, 4), ("rows_0", "rows_1", "cols_0", "cols_1"))
    placed = (
        P(ROWS, COLS),
        P(ROWS, None),
        P(None, COLS),
        P(ROWS, COLS),
        P(ROWS, None),
        P(None, COLS),
        P(COLS, ROWS),
        P(COLS, None),
        P(None, ROWS),
        P(ROWS_COLS),
        P(ROWS_COLS),
    )

    return jax.shard_map(
        local,
        mesh=torus,
        in_specs=placed,
        out_specs=(P(None, COLS), P(None, COLS), P(COLS, None), P()),
        check_vma=False,
    )
```
